8 devices in a mesh: dp: 2 (over z, y), tp: 4 (over x, core).
Axes of the slice: x: 2, y: 2, z: 1, core: 2. Of those that a mesh axis runs over, the one named last changes fastest.
Arguments:
- hidden: bfloat16 [1024, 5120], P('dp'), parts along dimension 0
- w_q: bfloat16 [5120, 5120], P(None, 'tp')
- w_k: bfloat16 [5120, 5120], P(None, 'tp')
- w_v: bfloat16 [5120, 5120], P(None, 'tp')
- w_o: bfloat16 [5120, 5120], P('tp')
- q_norm_w: float32 [5120], P('tp')
- k_norm_w: float32 [5120], P('tp')
- post_norm_w: float32 [5120], replicated
- k_cache: bfloat16 [1024, 32, 40, 128], P('dp', None, 'tp'), parts along dimension 0
- v_cache: bfloat16 [1024, 32, 40, 128], P('dp', None, 'tp'), parts along dimension 0
- positions: int32 [1024], P('dp'), parts along dimension 0
Outputs:
- output 1: bfloat16 [1024, 5120], P('dp'), parts along dimension 0
- output 2: bfloat16 [1024, 32, 40, 128], P('dp', None, 'tp'), parts along dimension 0
- output 3: bfloat16 [1024, 32, 40, 128], P('dp', None, 'tp'), parts along dimension 0
There are 2 independent parts. The reference program is written for one: setup_inputs(seed, part) draws one part's arguments, and reference() takes and returns one part's arrays. A program takes and returns all parts, laid end to end along the dimension named above; an argument that names none is the same for every part.
All inputs are finite; a program needn't handle non-finite values.
Results may differ from the reference program's by a relative error of at most 0.0104764.
Values are sent between devices in bfloat16 or wider.
A program may use at most 1 GiB of HBM per device.

```python
import jax
import jax.numpy as jnp
from jax import lax

BATCH = 512
CACHE_LEN = 32
HEADS = 40
HEAD_DIM = 128
WIDTH = HEADS * HEAD_DIM
NORM_EPS = 1e-6
ROPE_BASE = 500000.0


def setup_inputs(seed: int = 0, part: int = 0) -> dict:
    base_key = jax.random.key(seed)
    shared_keys = jax.random.split(base_key, 9)
    part_keys = jax.random.split(jax.random.fold_in(base_key, part), 6)
    fan_scale = WIDTH ** -0.5
    head_frac = jnp.arange(HEADS, dtype=jnp.float32) / max(HEADS - 1, 1)
    q_heads = jnp.exp(1.2 * (2.0 * head_frac - 1.0) + 0.2 * jax.random.normal(shared_keys[0], (HEADS,)))
    k_heads = jnp.exp(1.2 * (1.0 - 2.0 * head_frac) + 0.2 * jax.random.normal(shared_keys[1], (HEADS,)))
    q_cols = jnp.repeat(q_heads, HEAD_DIM)
    k_cols = jnp.repeat(k_heads, HEAD_DIM)
    w_q = (jax.random.normal(shared_keys[2], (WIDTH, WIDTH)) * fan_scale * q_cols[None, :]).astype(jnp.bfloat16)
    w_k = (jax.random.normal(shared_keys[3], (WIDTH, WIDTH)) * fan_scale * k_cols[None, :]).astype(jnp.bfloat16)
    w_v = (jax.random.normal(shared_keys[4], (WIDTH, WIDTH)) * fan_scale).astype(jnp.bfloat16)
    w_o = (jax.random.normal(shared_keys[5], (WIDTH, WIDTH)) * fan_scale).astype(jnp.bfloat16)
    q_norm_w = jax.random.uniform(shared_keys[6], (WIDTH,), minval=0.5, maxval=1.5).astype(jnp.float32)
    k_norm_w = jax.random.uniform(shared_keys[7], (WIDTH,), minval=0.5, maxval=1.5).astype(jnp.float32)
    post_norm_w = jax.random.uniform(shared_keys[8], (WIDTH,), minval=0.5, maxval=1.5).astype(jnp.float32)
    hidden = jax.random.normal(part_keys[0], (BATCH, WIDTH)).astype(jnp.bfloat16)
    k_cache = jax.random.normal(part_keys[1], (BATCH, CACHE_LEN, HEADS, HEAD_DIM)).astype(jnp.bfloat16)
    v_cache = jax.random.normal(part_keys[2], (BATCH, CACHE_LEN, HEADS, HEAD_DIM)).astype(jnp.bfloat16)
    slot_draw = jax.random.randint(part_keys[3], (BATCH,), 0, CACHE_LEN, dtype=jnp.int32)
    shift_bits = jax.random.randint(part_keys[4], (BATCH,), 0, 10, dtype=jnp.int32)
    longest = jax.random.randint(part_keys[5], (), 0, BATCH, dtype=jnp.int32)
    positions = jnp.where(jnp.arange(BATCH, dtype=jnp.int32) == longest, CACHE_LEN - 1, jnp.right_shift(slot_draw, shift_bits)).astype(jnp.int32)
    return dict(hidden=hidden, w_q=w_q, w_k=w_k, w_v=w_v, w_o=w_o, q_norm_w=q_norm_w, k_norm_w=k_norm_w, post_norm_w=post_norm_w, k_cache=k_cache, v_cache=v_cache, positions=positions)


def width_norm(vals, gain):
    wide = vals.astype(jnp.float32)
    inv_rms = lax.rsqrt(jnp.mean(wide * wide, axis=-1, keepdims=True) + NORM_EPS)
    return wide * inv_rms * gain


def apply_rope(heads_val, positions):
    half = HEAD_DIM // 2
    inv_freq = ROPE_BASE ** (-2.0 * jnp.arange(half, dtype=jnp.float32) / HEAD_DIM)
    angles = positions.astype(jnp.float32)[:, None, None] * inv_freq[None, None, :]
    cos_tab = jnp.cos(angles)
    sin_tab = jnp.sin(angles)
    wide = heads_val.astype(jnp.float32)
    first = wide[..., :half]
    second = wide[..., half:]
    return jnp.concatenate([first * cos_tab - second * sin_tab, second * cos_tab + first * sin_tab], axis=-1).astype(jnp.bfloat16)


def attend_row(row_args):
    q_row, k_row, v_row, row_pos = row_args
    slot_ids = jnp.arange(CACHE_LEN)
    scores = jnp.einsum('hd,shd->hs', q_row.astype(jnp.float32), k_row.astype(jnp.float32)) * HEAD_DIM ** -0.5
    scores = jnp.where(slot_ids[None, :] <= row_pos, scores, -1e30)
    probs = jax.nn.softmax(scores, axis=-1).astype(jnp.bfloat16)
    return jnp.einsum('hs,shd->hd', probs.astype(jnp.float32), v_row.astype(jnp.float32)).astype(jnp.bfloat16)


def reference(hidden, w_q, w_k, w_v, w_o, q_norm_w, k_norm_w, post_norm_w, k_cache, v_cache, positions):
    n_rows = hidden.shape[0]
    q_full = jnp.dot(hidden, w_q, preferred_element_type=jnp.float32).astype(jnp.bfloat16)
    k_full = jnp.dot(hidden, w_k, preferred_element_type=jnp.float32).astype(jnp.bfloat16)
    v_full = jnp.dot(hidden, w_v, preferred_element_type=jnp.float32).astype(jnp.bfloat16)
    q_normed = width_norm(q_full, q_norm_w).astype(jnp.bfloat16).reshape(n_rows, HEADS, HEAD_DIM)
    k_normed = width_norm(k_full, k_norm_w).astype(jnp.bfloat16).reshape(n_rows, HEADS, HEAD_DIM)
    q_rot = apply_rope(q_normed, positions)
    k_rot = apply_rope(k_normed, positions)
    v_heads = v_full.reshape(n_rows, HEADS, HEAD_DIM)
    at_slot = (jnp.arange(CACHE_LEN)[None, :] == positions[:, None])[:, :, None, None]
    k_new = jnp.where(at_slot, k_rot[:, None], k_cache)
    v_new = jnp.where(at_slot, v_heads[:, None], v_cache)
    attn = lax.map(attend_row, (q_rot, k_new, v_new, positions))
    a_out = jnp.dot(attn.reshape(n_rows, WIDTH), w_o, preferred_element_type=jnp.float32)
    hidden_out = (hidden.astype(jnp.float32) + width_norm(a_out, post_norm_w)).astype(jnp.bfloat16)
    return hidden_out, k_new, v_new
```

```python
import functools

import jax
import jax.numpy as jnp
import numpy as np
from jax import lax
from jax.experimental import pallas as pl
from jax.experimental.pallas import tpu as pltpu
from jax.sharding import PartitionSpec as P

NORM_EPS = 1e-6
ROPE_BASE = 500000.0
MESH = pl.DeviceIdType.MESH
ANY = pl.BlockSpec(memory_space=pl.ANY)
VMEM = pl.BlockSpec(memory_space=pltpu.VMEM)
HBM = pl.BlockSpec(memory_space=pltpu.HBM)
SMEM = pl.BlockSpec(memory_space=pltpu.SMEM)
BF = jnp.bfloat16
F32 = jnp.float32


def qkv_kernel(tp, hid_hbm, wq, wk, wv, wo, qn_hbm, kn_hbm, pos_hbm, q_out, k_out, v_out, w2,
               hid, wbuf, acc, epart, esend, erecv, cosd, sind, inv, qn, kn, pos, hsem, wsem, ssem, rsem, xsem, msem):
    rows, width = hid.shape
    nblk = acc.shape[0] // 2
    bn = acc.shape[2]
    ring = wbuf.shape[0]
    me = lax.axis_index("tp")
    barrier = pltpu.get_barrier_semaphore()
    for d in range(1, tp):
        pl.semaphore_signal(barrier, inc=1, device_id={"tp": lax.rem(me + d, tp)}, device_id_type=MESH)

    small = [pltpu.make_async_copy(src, dst, msem.at[n])
             for n, (src, dst) in enumerate(((pos_hbm, pos), (qn_hbm, qn), (kn_hbm, kn)))]
    for c in small:
        c.start()

    def fetch(src, j, i):
        cols = pl.ds(pl.multiple_of(j * bn, bn), bn)
        slot = lax.rem(i, ring)
        pltpu.make_async_copy(src.at[:, cols], wbuf.at[slot], wsem.at[slot]).start()

    def start(i):
        @pl.when(i < nblk)
        def _():
            fetch(wq, i, i)

        @pl.when(jnp.logical_and(i >= nblk, i < 2 * nblk))
        def _():
            fetch(wk, i - nblk, i)

        @pl.when(jnp.logical_and(i >= 2 * nblk, i < 3 * nblk))
        def _():
            fetch(wv, i - 2 * nblk, i)

    hid_copy = pltpu.make_async_copy(hid_hbm, hid, hsem)
    hid_copy.start()
    for i in range(ring - 1):
        start(jnp.int32(i))

    for c in small:
        c.wait()

    def spread(t, carry):
        rsl = pl.ds(pl.multiple_of(t * 8, 8), 8)
        cosd[rsl, :] = jnp.concatenate([jnp.full((1, 128), pos[t * 8 + r], jnp.int32) for r in range(8)], axis=0).astype(F32)
        return carry

    lax.fori_loop(0, rows // 8, spread, 0)
    lane = lax.broadcasted_iota(jnp.int32, cosd.shape, 1)
    pair = (lane % 64).astype(F32)
    angles = cosd[...] * jnp.exp(pair * np.float32(-2.0 * np.log(ROPE_BASE) / 128))
    cosd[...] = jnp.cos(angles)
    sin_tab = jnp.sin(angles)
    sind[...] = jnp.where(lane < angles.shape[1] // 2, -sin_tab, sin_tab)
    epart[...] = jnp.zeros_like(epart)
    hid_copy.wait()

    def block(i):
        slot = lax.rem(i, ring)
        start(i + ring - 1)
        pltpu.make_async_copy(wq.at[:, pl.ds(0, bn)], wbuf.at[slot], wsem.at[slot]).wait()
        return jnp.dot(hid[...], wbuf[slot], preferred_element_type=F32).astype(BF)

    core = lax.rem(me, 2)
    half = w2.shape[1]
    local = wo.shape[0]
    keep = pltpu.make_async_copy(wo.at[:, pl.ds(pl.multiple_of(core * half, 128), half)], w2.at[pl.ds(0, local)], xsem.at[2])
    swap = pltpu.make_async_remote_copy(
        src_ref=wo.at[:, pl.ds(pl.multiple_of((1 - core) * half, 128), half)], dst_ref=w2.at[pl.ds(local, local)],
        send_sem=xsem.at[0], recv_sem=xsem.at[1], device_id={"tp": me + 1 - 2 * core}, device_id_type=MESH)

    def qk_step(i, carry):
        @pl.when(i == 2)
        def _():
            pl.semaphore_wait(barrier, tp - 1)
            swap.start()
            keep.start()

        res = block(i)
        acc[i] = res
        wide = res.astype(F32)
        sq = wide * wide
        part = sq[:, :128]
        for c in range(1, bn // 128):
            part += sq[:, c * 128:(c + 1) * 128]
        epart[i // nblk] += part
        return carry

    lax.fori_loop(0, 2 * nblk, qk_step, 0)

    for s in range(2):
        esend[s:s + 1, :] = jnp.sum(epart[s].T, axis=0, keepdims=True)

    def copy_to(d):
        return pltpu.make_async_remote_copy(
            src_ref=esend, dst_ref=erecv.at[d - 1], send_sem=ssem.at[d - 1], recv_sem=rsem.at[d - 1],
            device_id={"tp": lax.rem(me + d, tp)}, device_id_type=MESH)

    def v_step(i, carry):
        res = block(i)

        @pl.when(i == 2 * nblk)
        def _():
            for d in range(1, tp):
                copy_to(d).start()

        v_out[:, pl.ds(pl.multiple_of((i - 2 * nblk) * bn, bn), bn)] = res
        return carry

    lax.fori_loop(2 * nblk, 3 * nblk, v_step, 0)

    energy = esend[...]
    for d in range(1, tp):
        copy_to(d).wait()
        energy = energy + erecv[d - 1]
    inv_row = lax.rsqrt(energy / width + NORM_EPS)
    inv[...] = inv_row.T

    rb = 64
    per = bn // 128

    def finish(t, carry):
        rsl = pl.ds(pl.multiple_of(t * rb, rb), rb)
        cos_t = cosd[rsl, :]
        sin_t = sind[rsl, :]
        scale = inv[rsl, :]
        for s, gain, out in ((0, qn, q_out), (1, kn, k_out)):
            sc = scale[:, s:s + 1]
            for h in range(nblk * per):
                csl = slice(h * 128, (h + 1) * 128)
                x = acc[s * nblk + h // per, rsl, (h % per) * 128:(h % per + 1) * 128].astype(F32)
                y = (x * sc * gain[csl][None]).astype(BF).astype(F32)
                out[rsl, csl] = (y * cos_t + pltpu.roll(y, 64, 1) * sin_t).astype(BF)
        return carry

    lax.fori_loop(0, rows // rb, finish, 0)
    swap.wait()
    keep.wait()


def qkv_project(tp, hidden, w_q, w_k, w_v, w_o, q_norm_w, k_norm_w, positions):
    rows, width = hidden.shape
    local = w_q.shape[1]
    bn = 256
    ring = 3
    out = pltpu.VMEM((rows, local), BF)
    return pl.pallas_call(
        functools.partial(qkv_kernel, tp),
        out_shape=(out, out, out, pltpu.VMEM((2 * local, width // 2), BF)),
        in_specs=[HBM] * 8,
        out_specs=(VMEM, VMEM, VMEM, VMEM),
        scratch_shapes=[
            pltpu.VMEM((rows, width), BF),
            pltpu.VMEM((ring, width, bn), BF),
            pltpu.VMEM((2 * local // bn, rows, bn), BF),
            pltpu.VMEM((2, rows, 128), F32),
            pltpu.VMEM((8, rows), F32),
            pltpu.VMEM((tp - 1, 8, rows), F32),
            pltpu.VMEM((rows, 128), F32),
            pltpu.VMEM((rows, 128), F32),
            pltpu.VMEM((rows, 8), F32),
            pltpu.VMEM((local,), F32),
            pltpu.VMEM((local,), F32),
            pltpu.SMEM((rows,), jnp.int32),
            pltpu.SemaphoreType.DMA,
            pltpu.SemaphoreType.DMA((ring,)),
            pltpu.SemaphoreType.DMA((tp - 1,)),
            pltpu.SemaphoreType.DMA((tp - 1,)),
            pltpu.SemaphoreType.DMA((3,)),
            pltpu.SemaphoreType.DMA((3,)),
        ],
        compiler_params=pltpu.CompilerParams(collective_id=0, has_side_effects=True, vmem_limit_bytes=50000000),
        cost_estimate=pl.CostEstimate(flops=6 * rows * width * local, bytes_accessed=6 * width * local, transcendentals=0),
        name="qkv",
    )(hidden, w_q, w_k, w_v, w_o, q_norm_w, k_norm_w, positions)


def attend_kernel(row0, rows, rb, ring, pos, qb, kb, vb, kc, vc, *refs):
    o_ref, ko, vo, kbuf, vbuf, q_rows, k_rows, v_rows, o_rows, isem, osem = refs[-11:]
    heads, slots = kbuf.shape[2], kbuf.shape[3]
    nblk = rows // rb
    scale = 128.0 ** -0.5

    def ins(b, slot):
        rsl = pl.ds(row0 + b * rb, rb)
        return (pltpu.make_async_copy(kc.at[rsl], kbuf.at[slot], isem.at[0, slot]),
                pltpu.make_async_copy(vc.at[rsl], vbuf.at[slot], isem.at[1, slot]))

    def outs(b, slot):
        rsl = pl.ds(row0 + b * rb, rb)
        return (pltpu.make_async_copy(kbuf.at[slot], ko.at[rsl], osem.at[0, slot]),
                pltpu.make_async_copy(vbuf.at[slot], vo.at[rsl], osem.at[1, slot]))

    ahead = (2 * ring) // 3
    for b in range(min(ahead, nblk)):
        for c in ins(b, b):
            c.start()

    head_i = lax.broadcasted_iota(jnp.int32, (16, 128), 0)
    lane_i = lax.broadcasted_iota(jnp.int32, (16, 128), 1)
    slot_of = jnp.where((lane_i // slots) == (head_i % 4), lane_i % slots, 1 << 20)
    tile_of = head_i // 4
    sub_i = lax.broadcasted_iota(jnp.int32, (16, 128), 0)
    q_rows[...] = jnp.zeros_like(q_rows)

    def step(b, carry):
        slot = lax.rem(b, ring)

        @pl.when(b + ahead < nblk)
        def _():
            nslot = lax.rem(b + ahead, ring)

            @pl.when(b + ahead >= ring)
            def _():
                for c in outs(b, nslot):
                    c.wait()

            for c in ins(b + ahead, nslot):
                c.start()

        rsl = pl.ds(pl.multiple_of(b * rb, rb), rb)
        gsl = pl.ds(pl.multiple_of(row0 + b * rb, rb), rb)
        for h in range(heads):
            csl = slice(h * 128, (h + 1) * 128)
            q_rows[:, h, :] = qb[gsl, csl].astype(F32)
            k_rows[:, h, :] = kb[gsl, csl].astype(F32)
            v_rows[:, h, :] = vb[gsl, csl].astype(F32)
        for c in ins(b, slot):
            c.wait()
        kbs, vbs = kbuf.at[slot], vbuf.at[slot]

        def insert(g, carry):
            todo = []
            for i in range(2):
                r = g * 2 + i
                p = pos[row0 + b * rb + r]
                tsl = pl.ds(pl.multiple_of((p // 16) * 16, 16), 16)
                here = sub_i == (p % 16)
                for h in range(heads):
                    for src, dst in ((k_rows, kbs), (v_rows, vbs)):
                        todo.append((r, h, tsl, here, src, dst, dst[r, h, tsl, :]))
            for r, h, tsl, here, src, dst, old in todo:
                new = jnp.broadcast_to(src[r, h:h + 1, :], (16, 128)).astype(BF)
                dst[r, h, tsl, :] = jnp.where(here, new, old)
            return carry

        lax.fori_loop(0, rb // 2, insert, 0)
        for c in outs(b, slot):
            c.start()

        raw = []
        for r in range(rb):
            keys = kbs[r].reshape(heads * slots, 128)
            s = lax.dot_general(q_rows[r].astype(BF), keys, (((1,), (1,)), ((), ())), preferred_element_type=F32)
            third = jnp.concatenate([s[:, 256:320], s[:, 256:320]], axis=1)
            raw.append(jnp.where(tile_of == 0, s[:, :128], jnp.where(tile_of == 1, s[:, 128:256], third)))
        raw = [jnp.where(slot_of <= pos[row0 + b * rb + r], raw[r] * scale, -1e30) for r in range(rb)]
        tops = [jnp.max(s, axis=1, keepdims=True) for s in raw]
        exps = [jnp.exp(s - m) for s, m in zip(raw, tops)]
        sums = [jnp.sum(e, axis=1, keepdims=True) for e in exps]
        probs = [e * (1.0 / t) for e, t in zip(exps, sums)]
        mixed = []
        for pr in probs:
            pieces = [jnp.where(tile_of == t, pr, 0.0).astype(BF) for t in range(3)]
            mixed.append(jnp.concatenate([pieces[0], pieces[1], pieces[2][:, :64]], axis=1))
        for r in range(rb):
            o_rows[r] = jnp.dot(mixed[r], vbs[r].reshape(heads * slots, 128), preferred_element_type=F32)
        for h in range(heads):
            o_ref[rsl, h * 128:(h + 1) * 128] = o_rows[:, h, :].astype(BF)
        return carry

    lax.fori_loop(0, nblk, step, 0)
    for b in range(max(0, nblk - ring), nblk):
        for c in outs(b, b % ring):
            c.wait()


def attend(row0, rows, positions, q, k, v, kc, vc, prev):
    heads, slots = kc.shape[1], kc.shape[2]
    local = q.shape[1]
    rb, ring = 8, 12
    cache = jax.ShapeDtypeStruct(kc.shape, BF)
    args = [positions, q, k, v, kc, vc]
    aliases = {}
    if prev is not None:
        args += list(prev)
        aliases = {6: 1, 7: 2}
    return pl.pallas_call(
        functools.partial(attend_kernel, row0, rows, rb, ring),
        out_shape=(jax.ShapeDtypeStruct((rows, local), BF), cache, cache),
        in_specs=[SMEM, VMEM, VMEM, VMEM] + [HBM] * (len(args) - 4),
        out_specs=(VMEM, HBM, HBM),
        scratch_shapes=[
            pltpu.VMEM((ring, rb, heads, slots, 128), BF),
            pltpu.VMEM((ring, rb, heads, slots, 128), BF),
            pltpu.VMEM((rb, 16, 128), F32),
            pltpu.VMEM((rb, 16, 128), F32),
            pltpu.VMEM((rb, 16, 128), F32),
            pltpu.VMEM((rb, 16, 128), F32),
            pltpu.SemaphoreType.DMA((2, ring)),
            pltpu.SemaphoreType.DMA((2, ring)),
        ],
        input_output_aliases=aliases,
        compiler_params=pltpu.CompilerParams(vmem_limit_bytes=24 * 2**20),
        cost_estimate=pl.CostEstimate(flops=200 * rows * local * slots, bytes_accessed=8 * rows * local * slots, transcendentals=0),
        name="attend",
    )(*args)


def proj_kernel(o, w2, s_out, osib, part, ssem, rsem):
    rows, local = o.shape
    half = s_out.shape[1]
    me = lax.axis_index("tp")
    core = lax.rem(me, 2)
    peer = {"tp": me + 1 - 2 * core}
    barrier = pltpu.get_barrier_semaphore()
    pl.semaphore_signal(barrier, inc=1, device_id=peer, device_id_type=MESH)
    pl.semaphore_wait(barrier, 1)
    swap = pltpu.make_async_remote_copy(src_ref=o, dst_ref=osib, send_sem=ssem, recv_sem=rsem,
                                        device_id=peer, device_id_type=MESH)
    swap.start()
    bn = 512

    def own(j, carry):
        cols = pl.ds(pl.multiple_of(j * bn, bn), bn)
        part[j] = jnp.dot(o[...], w2[0:local, cols], preferred_element_type=F32)
        return carry

    lax.fori_loop(0, half // bn, own, 0)
    swap.wait()

    def both(j, carry):
        cols = pl.ds(pl.multiple_of(j * bn, bn), bn)
        s_out[:, cols] = (part[j] + jnp.dot(osib[...], w2[local:2 * local, cols], preferred_element_type=F32)).astype(BF)
        return carry

    lax.fori_loop(0, half // bn, both, 0)


def project(cid, o, w2):
    rows, local = o.shape
    half = w2.shape[1]
    return pl.pallas_call(
        proj_kernel,
        out_shape=jax.ShapeDtypeStruct((rows, half), BF),
        in_specs=[VMEM, VMEM],
        out_specs=VMEM,
        scratch_shapes=[
            pltpu.VMEM((rows, local), BF),
            pltpu.VMEM((half // 512, rows, 512), F32),
            pltpu.SemaphoreType.DMA,
            pltpu.SemaphoreType.DMA,
        ],
        compiler_params=pltpu.CompilerParams(collective_id=cid, has_side_effects=True, vmem_limit_bytes=20 * 2**20),
        cost_estimate=pl.CostEstimate(flops=4 * rows * local * half, bytes_accessed=6 * local * half, transcendentals=0),
        name="proj",
    )(o, w2)


def final_kernel(s, r, s_sib, r_sib, hid, gain, *refs):
    out = refs[-1]
    half = s.shape[1]
    core = lax.rem(lax.axis_index("tp"), 2)
    mine = pl.ds(pl.multiple_of(core * half, 128), half)
    other = pl.ds(pl.multiple_of((1 - core) * half, 128), half)
    a = s[...].astype(F32) + r[...].astype(F32)
    b = s_sib[...].astype(F32) + r_sib[...].astype(F32)
    energy = jnp.sum(a * a, axis=1, keepdims=True) + jnp.sum(b * b, axis=1, keepdims=True)
    inv = lax.rsqrt(energy / (2 * half) + NORM_EPS)
    out[:, mine] = (hid[:, mine].astype(F32) + a * inv * gain[:, mine]).astype(BF)
    out[:, other] = (hid[:, other].astype(F32) + b * inv * gain[:, other]).astype(BF)


def finish_rows(row0, s, r, s_sib, r_sib, hidden, gain, prev):
    rows, half = s.shape
    rb = 32
    part = pl.BlockSpec((rb, half), lambda i: (i, 0))
    whole = pl.BlockSpec((rb, 2 * half), lambda i: (i + row0 // rb, 0))
    args = [s, r, s_sib, r_sib, hidden, gain]
    aliases = {}
    specs = [part] * 4 + [whole, pl.BlockSpec((1, 2 * half), lambda i: (0, 0))]
    if prev is not None:
        args.append(prev)
        specs.append(ANY)
        aliases = {6: 0}
    return pl.pallas_call(
        final_kernel,
        out_shape=jax.ShapeDtypeStruct(hidden.shape, BF),
        grid=(rows // rb,),
        in_specs=specs,
        out_specs=whole,
        input_output_aliases=aliases,
        compiler_params=pltpu.CompilerParams(vmem_limit_bytes=16 * 2**20),
        cost_estimate=pl.CostEstimate(flops=40 * rows * half, bytes_accessed=16 * rows * half, transcendentals=0),
        name="final",
    )(*args)


CHUNKS = (128, 128, 128, 128)


def solution(mesh):
    tp = mesh.shape["tp"]
    across = [(i, (i + 2) % tp) for i in range(tp)]
    inside = [(i, i ^ 1) for i in range(tp)]

    def local_step(hidden, w_q, w_k, w_v, w_o, q_norm_w, k_norm_w, post_norm_w, k_cache, v_cache, positions):
        q, k, v, w2 = qkv_project(tp, hidden, w_q, w_k, w_v, w_o, q_norm_w, k_norm_w, positions)
        kc = k_cache.transpose(0, 2, 1, 3)
        vc = v_cache.transpose(0, 2, 1, 3)
        gain = post_norm_w[None]
        caches, row0, out, waiting = None, 0, None, []
        for n, rows in enumerate(CHUNKS):
            o, *caches = attend(row0, rows, positions, q, k, v, kc, vc, caches)
            s = project(1 + n, o, w2)
            r = lax.ppermute(s, "tp", across)
            s_sib = lax.ppermute(s, "tp", inside)
            if n == len(CHUNKS) - 1:
                for first, *parts in waiting:
                    out = finish_rows(first, *parts, hidden, gain, out)
                r, out = lax.optimization_barrier((r, out))
            r_sib = lax.ppermute(r, "tp", inside)
            waiting.append((row0, s, r, s_sib, r_sib))
            row0 += rows
        out = finish_rows(*waiting[-1], hidden, gain, out)
        return out, caches[0].transpose(0, 2, 1, 3), caches[1].transpose(0, 2, 1, 3)

    cache_spec = P("dp", None, "tp", None)
    return jax.shard_map(
        local_step, mesh=mesh,
        in_specs=(P("dp", None), P(None, "tp"), P(None, "tp"), P(None, "tp"), P("tp", None), P("tp"), P("tp"), P(None),
                  cache_spec, cache_spec, P("dp")),
        out_specs=(P("dp", None), cache_spec, cache_spec), check_vma=False)
```
